32 devices in a mesh: rows: 8 (over z, x), cols: 4 (over y, core).
Axes of the slice: x: 2, y: 2, z: 4, core: 2. Of those that a mesh axis runs over, the one named last changes fastest.
Arguments:
- panel_t: float32 [16, 2048], P(None, ('rows', 'cols')), may hold values from -6 to 6
- kinship: float32 [2048, 2048], P('rows', 'cols'), may hold values from -0.125 to 0.125
Outputs:
- kin_panel_t: float32 [16, 2048], P(None, ('rows', 'cols'))
- score: float32 [16, 16], replicated
The draws below stay inside these ranges and needn't reach their ends.
All inputs are finite; a program needn't handle non-finite values.
Results may differ from the reference program's by a relative error of at most 0.00008.
Values sent between devices are 32-bit elements; how exact they have to be, the bound alone decides.
A program may use at most 64 MiB of HBM per device.

```python
import jax
import jax.numpy as jnp
from jax import lax

TRAITS = 16
SAMPLES = 2048


def block_levels(rng, shape, pieces, smallest, largest):
    loudness, own = 1.0, jax.random.fold_in(rng, 6)
    for dim, parts in pieces:
        heights = jnp.exp(jax.random.uniform(jax.random.fold_in(own, dim), (parts,), jnp.float32, smallest / len(pieces), largest / len(pieces)))
        loudness = loudness * jnp.repeat(heights, shape[dim] // parts).reshape([-1 if axis == dim else 1 for axis in range(len(shape))])
    return loudness


def centred(key, shape, scale, most, pieces=(), dtype=jnp.bfloat16):
    factor_of = block_levels(key, shape, pieces, -0.22, 0.18) if pieces else 1.0
    drawn = jax.random.normal(key, shape, jnp.float32) * scale * factor_of
    return jnp.minimum(jnp.maximum(drawn, -most), most).astype(dtype)


def setup_inputs(seed: int = 0) -> dict:
    streams_of = jax.random.split(jax.random.key(seed), 3)
    panel_t = centred(streams_of[0], (TRAITS, SAMPLES), 1.0, 6.0, ((1, 32),), jnp.float32)
    kinship = centred(streams_of[1], (SAMPLES, SAMPLES), SAMPLES ** -0.5, 0.125, ((0, 8), (1, 4)), jnp.float32)
    return dict(panel_t=panel_t, kinship=kinship)


def reference(panel_t, kinship):
    kin_panel_t = lax.dot_general(panel_t, kinship, (((1,), (1,)), ((), ())), precision=lax.Precision.HIGHEST, preferred_element_type=jnp.float32)
    score = lax.dot_general(panel_t, kin_panel_t, (((1,), (1,)), ((), ())), precision=lax.Precision.HIGHEST, preferred_element_type=jnp.float32)
    score = score / jnp.sqrt(jnp.float32(panel_t.shape[1]))
    return (kin_panel_t, score)
```

```python
import functools
import math

import jax
import jax.numpy as jnp
from jax import lax
from jax.experimental import pallas as pl
from jax.experimental.pallas import tpu as pltpu
from jax.sharding import PartitionSpec as P

MESH = pl.DeviceIdType.MESH
LANES = 128
SUBLANES = 8


def split(x):
    high = x.astype(jnp.bfloat16)
    rest = x - high.astype(jnp.float32)
    mid = rest.astype(jnp.bfloat16)
    low = (rest - mid.astype(jnp.float32)).astype(jnp.bfloat16)
    return high, mid, low


def dot(left, right, dims):
    n = left[0].shape[0]

    def one(pieces, weights):
        return lax.dot_general(
            jnp.concatenate(pieces, axis=0),
            weights,
            (dims, ((), ())),
            preferred_element_type=jnp.float32,
        )

    high, mid, low = one(left, right[0]), one(left[:2], right[1]), one(left[:1], right[2])
    small = high[2 * n :] + mid[n:] + low
    return high[:n] + (high[n : 2 * n] + mid[:n] + small)


def fold(x):
    half = x.shape[0] // 2
    return jnp.concatenate([x[:half], x[half:]], axis=1)


def unfold(x):
    own = x.shape[1] // 2
    return jnp.concatenate([x[:, :own], x[:, own:]], axis=0)


def join(chunks):
    own = chunks[0].shape[1] // 2
    return jnp.concatenate(
        [
            jnp.concatenate([x[:, :own] for x in chunks], axis=1),
            jnp.concatenate([x[:, own:] for x in chunks], axis=1),
        ],
        axis=0,
    )


def remote(src, dst, send, recv, where):
    return pltpu.make_async_remote_copy(
        src_ref=src,
        dst_ref=dst,
        send_sem=send,
        recv_sem=recv,
        device_id=where,
        device_id_type=MESH,
    )


def kernel(
    rows,
    cols,
    panel_hbm,
    kin_hbm,
    out_ref,
    score_ref,
    loaded,
    panel,
    kin,
    kin_high,
    kin_mid,
    kin_low,
    slab,
    block,
    part,
    landed,
    side,
    sides,
    samples,
    form,
    forms,
    total,
    panel_sem,
    kin_sem,
    slab_send,
    slab_recv,
    block_send,
    block_recv,
    relay_send,
    part_send,
    part_recv,
    side_send,
    side_recv,
    sample_send,
    sample_recv,
    form_send,
    forms_recv,
    last_send,
    total_send,
    total_recv,
):
    count = rows * cols
    depth = rows // cols
    plane = depth * cols
    traits, own = panel_hbm.shape
    row, col = lax.axis_index("rows"), lax.axis_index("cols")
    me = row * cols + col
    zz, xx = row // depth, row % depth
    mine = me % plane

    late = zz > col
    early = zz <= col
    diagonal = zz == col
    first = (row == 0) & (col == 0)
    root = (row == 0) & (col == 1)
    n_early = depth * (cols * (cols + 1) // 2)
    starts = [depth * (c * (cols - 1) - c * (c - 1) // 2) for c in range(cols)]
    early_slot = (col * (col + 1) // 2 + zz) * depth + xx
    late_slot = depth * (col * (cols - 1) - col * (col - 1) // 2 + zz - col - 1) + xx
    to_first, to_root = (0, 0), (0, 1)

    barrier = pltpu.get_barrier_semaphore()

    def greet(where):
        pl.semaphore_signal(barrier, inc=1, device_id=where, device_id_type=MESH)

    def each_row(low, high, body):
        def step(r, carry):
            body(r)
            return carry

        lax.fori_loop(low, high, step, 0)

    for step in range(1, cols):
        greet((row, (col + step) % cols))

    @pl.when(late)
    def _():
        greet((col * depth + xx, col))

    @pl.when(early)
    def _():
        def body(r):
            for c in range(cols):

                @pl.when((r != row) | (col != c))
                def _():
                    greet((r, c))

        each_row(col * depth, col * depth + depth, body)

    @pl.when(first | root)
    def _():
        def body(r):
            for c in range(cols):
                greet((r, c))

        each_row(1, rows, body)

    get_panel = pltpu.make_async_copy(panel_hbm, loaded, panel_sem)
    get_panel.start()
    get_kin = pltpu.make_async_copy(kin_hbm, kin, kin_sem)
    get_kin.start()
    get_panel.wait()
    panel[...] = fold(loaded[...])
    slab[col] = panel[...]
    pl.semaphore_wait(
        barrier,
        (cols - 1)
        + (zz + 1) * depth
        + jnp.where(diagonal, cols - 2 - zz, 0)
        + jnp.where(row > 0, 2, 0),
    )

    for step in range(1, cols):
        c = (col + step) % cols
        remote(panel, slab.at[col], slab_send, slab_recv, (row, c)).start()

    def to_block(r):
        @pl.when((r != row) | (col != zz))
        def _():
            remote(panel, block.at[mine], block_send, block_recv, (r, zz)).start()

    each_row(0, zz * depth + depth, to_block)
    keep_block = pltpu.make_async_copy(panel, block.at[mine], block_recv)
    send_sample = remote(panel, samples.at[me], sample_send, sample_recv, to_root)
    sampled = (zz < cols - 1) & ((row != 0) | (col != 1))

    @pl.when(diagonal)
    def _():
        keep_block.start()

    @pl.when(sampled)
    def _():
        send_sample.start()

    @pl.when(root)
    def _():
        samples[1] = panel[...]

    def wait_bytes(ref, sem):
        pltpu.make_async_copy(ref, ref, sem).wait()

    get_kin.wait()
    kin_high[...], kin_mid[...], kin_low[...] = split(kin[...])
    wait_bytes(slab.at[pl.ds(0, cols - 1)], slab_recv)
    weights = (kin_high[...], kin_mid[...], kin_low[...])
    slab_panel = join([slab[c] for c in range(cols)])
    value = dot(split(slab_panel / math.sqrt(count * own)), weights, ((1,), (0,)))
    side[...] = value
    send_side = remote(
        side, sides.at[late_slot], side_send, side_recv.at[col], to_root
    )

    @pl.when(late)
    def _():
        send_side.start()

    def widen(x):
        return tuple(jnp.concatenate([p] * (LANES // traits), axis=0) for p in split(x))

    sublane = lax.broadcasted_iota(jnp.int32, (traits, LANES), 0) % SUBLANES
    group = lax.broadcasted_iota(jnp.int32, (traits, LANES), 1) // traits

    def form_of(panels, wide):
        spread = dot(panels, wide, ((1,), (1,)))
        spread = jnp.where(sublane == group, spread, 0.0)
        return jnp.sum(spread.reshape(traits // SUBLANES, SUBLANES, LANES), axis=1)

    wide = widen(value)
    wait_bytes(block, block_recv)
    block_panel = split(join([block[m] for m in range(plane)]))
    form[...] = form_of(block_panel, wide)
    form_first = remote(form, forms.at[early_slot], form_send, forms_recv, to_first)
    form_root = remote(form, forms.at[early_slot], form_send, forms_recv, to_root)

    @pl.when(early & ((row != 0) | (col != 0)))
    def _():
        form_first.start()

    @pl.when(early & ((row != 0) | (col != 1)))
    def _():
        form_root.start()

    @pl.when(first)
    def _():
        forms[0] = form[...]

    @pl.when(root)
    def _():
        forms[depth] = form[...]

    @pl.when(diagonal)
    def _():
        def relay(z):
            where = (z * depth + xx, col)
            remote(block, block, relay_send, block_recv, where).start()

        each_row(zz + 1, cols, relay)

    value = dot(block_panel, (kin_high[...], kin_mid[...], kin_low[...]), ((1,), (1,)))
    for c in range(cols):
        part[c] = fold(value[:, c * own : (c + 1) * own])
    for step in range(1, cols):
        c = (col + step) % cols
        remote(part.at[c], landed.at[col], part_send, part_recv, (row, c)).start()
    landed[col] = part[col]

    send_last = remote(
        forms.at[n_early], forms.at[n_early], last_send, forms_recv, to_first
    )

    def to_all(r):
        for c in range(cols):

            @pl.when((r != 0) | (c > 1))
            def _():
                remote(total, total, total_send, total_recv, (r, c)).start()

    @pl.when(root)
    def _():
        wait_bytes(samples.at[pl.ds(0, plane * (cols - 1) - 1)], sample_recv)
        last = jnp.zeros((traits // SUBLANES, LANES), jnp.float32)
        for c in range(cols - 1):
            low, n = starts[c], starts[c + 1] - starts[c]
            panels = split(join([samples[c * plane + m] for m in range(plane)]))
            wait_bytes(sides.at[pl.ds(low, n)], side_recv.at[c])
            last += form_of(panels, widen(jnp.sum(sides[low : low + n], axis=0)))
        forms[n_early] = last
        send_last.start()
        wait_bytes(forms.at[pl.ds(0, n_early - 1)], forms_recv)
        total[...] = jnp.sum(forms[...], axis=0)
        each_row(0, rows, to_all)

    wait_bytes(landed.at[pl.ds(0, cols - 1)], part_recv)
    result = landed[0]
    for c in range(1, cols):
        result += landed[c]
    out_ref[...] = unfold(result)

    wait_bytes(slab.at[pl.ds(0, cols - 1)], slab_send)
    for z in range(cols):

        @pl.when((zz == z) & (col != z))
        def _():
            wait_bytes(block.at[pl.ds(0, (z + 1) * depth)], block_send)

        @pl.when((zz == z) & (col == z))
        def _():
            if (z + 1) * depth > 1:
                wait_bytes(block.at[pl.ds(0, (z + 1) * depth - 1)], block_send)

    @pl.when(diagonal)
    def _():
        each_row(zz + 1, cols, lambda z: wait_bytes(block, relay_send))

    @pl.when(sampled)
    def _():
        send_sample.wait_send()

    @pl.when(late)
    def _():
        send_side.wait_send()

    @pl.when(early & ((row != 0) | (col != 0)))
    def _():
        form_first.wait_send()

    @pl.when(early & ((row != 0) | (col != 1)))
    def _():
        form_root.wait_send()

    wait_bytes(landed.at[pl.ds(0, cols - 1)], part_send)

    @pl.when(root)
    def _():
        send_last.wait_send()
        for _ in range(cols - 2):
            wait_bytes(total, total_send)
        each_row(0, (rows - 1) * cols, lambda r: wait_bytes(total, total_send))

    @pl.when(first)
    def _():
        wait_bytes(forms.at[pl.ds(0, n_early)], forms_recv)
        total[...] = jnp.sum(forms[...], axis=0)

    @pl.when((row != 0) | (col > 1))
    def _():
        wait_bytes(total, total_recv)

    whole = total[...]
    spread = jnp.concatenate(
        [
            jnp.broadcast_to(whole[i : i + 1, :], (SUBLANES, LANES))
            for i in range(traits // SUBLANES)
        ],
        axis=0,
    )
    spread = jnp.where(sublane == group, spread, 0.0)
    score_ref[...] = jnp.sum(spread.T.reshape(LANES // traits, traits, traits), axis=0)


def finish(value_ref, form_ref, out_ref, score_ref, sems):
    first = pltpu.make_async_copy(value_ref, out_ref, sems.at[0])
    second = pltpu.make_async_copy(form_ref, score_ref, sems.at[1])
    first.start()
    second.start()
    first.wait()
    second.wait()


def shards(rows, cols, panel_t, kinship):
    traits, own = panel_t.shape
    plane = rows // cols * cols
    vmem = pltpu.VMEM
    dma = pltpu.SemaphoreType.DMA
    f32, bf16 = jnp.float32, jnp.bfloat16
    chunk = (traits // 2, 2 * own)
    form = (traits * traits // LANES, LANES)
    n_early = plane * (cols + 1) // 2
    n_late = plane * (cols - 1) // 2
    value, score = (
        pl.pallas_call(
            functools.partial(kernel, rows, cols),
            out_shape=(vmem((traits, own), f32), vmem((traits, traits), f32)),
            in_specs=[pl.BlockSpec(memory_space=pl.ANY)] * 2,
            out_specs=(pl.BlockSpec(memory_space=vmem),) * 2,
            scratch_shapes=[
                vmem((traits, own), f32),
                vmem(chunk, f32),
                vmem(kinship.shape, f32),
                vmem(kinship.shape, bf16),
                vmem(kinship.shape, bf16),
                vmem(kinship.shape, bf16),
                vmem((cols,) + chunk, f32),
                vmem((plane,) + chunk, f32),
                vmem((cols,) + chunk, f32),
                vmem((cols,) + chunk, f32),
                vmem((traits, kinship.shape[1]), f32),
                vmem((n_late, traits, kinship.shape[1]), f32),
                vmem((plane * (cols - 1),) + chunk, f32),
                vmem(form, f32),
                vmem((n_early + 1,) + form, f32),
                vmem(form, f32),
            ]
            + [dma(())] * 10
            + [dma((cols,))]
            + [dma(())] * 7,
            compiler_params=pltpu.CompilerParams(collective_id=0, has_side_effects=True),
        )(panel_t, kinship)
    )
    return tuple(
        pl.pallas_call(
            finish,
            out_shape=(
                jax.ShapeDtypeStruct((traits, own), f32),
                jax.ShapeDtypeStruct((traits, traits), f32),
            ),
            in_specs=[pl.BlockSpec(memory_space=pl.ANY)] * 2,
            out_specs=(pl.BlockSpec(memory_space=pl.ANY),) * 2,
            scratch_shapes=[dma((2,))],
            compiler_params=pltpu.CompilerParams(vmem_limit_bytes=1024 * 1024),
        )(value, score)
    )


def solution(mesh):
    rows, cols = mesh.shape["rows"], mesh.shape["cols"]
    return jax.shard_map(
        functools.partial(shards, rows, cols),
        mesh=mesh,
        in_specs=(P(None, ("rows", "cols")), P("rows", "cols")),
        out_specs=(P(None, ("rows", "cols")), P()),
        check_vma=False,
    )
```
